1024 devices in a mesh: pipe: 32 (over x, z_lo), expert: 32 (over y, z_hi, core).
Axes of the slice: x: 4, y: 4, z: 32 (z_hi: 4, z_lo: 8; z = z_hi * 8 + z_lo), core: 2. Of those that a mesh axis runs over, the one named last changes fastest.
Arguments:
- forward_in: bfloat16 [32, 2048, 3584], P('pipe', 'expert'), may hold values from -6 to 6
- forward_ids: int32 [32, 2048, 1], P('pipe', 'expert'), may hold values from 0 to 7, as said below
- forward_gates: float32 [32, 2048, 1], P('pipe', 'expert'), may hold values from 0.4 to 1
- grad_in: bfloat16 [32, 2048, 3584], P('pipe', 'expert'), may hold values from -6 to 6
- grad_ids: int32 [32, 2048, 1], P('pipe', 'expert'), may hold values from 0 to 7, as said below
- grad_gates: float32 [32, 2048, 1], P('pipe', 'expert'), may hold values from 0.4 to 1
- saved_input: bfloat16 [32, 2048, 3584], P('pipe', 'expert'), may hold values from -6 to 6
- saved_acts: bfloat16 [32, 32, 256, 512], P('pipe', 'expert'), may hold values from -8 to 8
- norm_gain: float32 [32, 3584], P('pipe'), may hold values from 0.1 to 1.9
- weight_in: bfloat16 [32, 3584, 512], P('expert'), may hold values from -0.09375 to 0.09375
- weight_out: bfloat16 [32, 256, 3584], P('expert'), may hold values from -0.1875 to 0.1875
Outputs:
- forward_out: bfloat16 [32, 2048, 3584], P('pipe', 'expert')
- grad_out: bfloat16 [32, 2048, 3584], P('pipe', 'expert')
The draws below stay inside these ranges and needn't reach their ends.
Inputs may be any that keep to these rules, and one draw needn't show every extreme that they name: `forward_ids`: A token's 1 ids are distinct; for each section, the 64 tokens of one device name every expert exactly 8 times. `grad_ids`: A token's 1 ids are distinct; for each section, the 64 tokens of one device name every expert exactly 8 times.
All inputs are finite; a program needn't handle non-finite values.
Results may differ from the reference program's by a relative error of at most 0.008.
Values may be sent and summed in bfloat16 or wider, within the bound.
No kernel may reach another device: no remote copies, remote signals or barrier semaphores. Data moves between devices by JAX's collectives and lax.ppermute only.
A program may use at most 32 MiB of HBM per device.

```python
import jax
import jax.numpy as jnp
from jax import lax

D = 3584
FFW = 1024
TOP = 1
TOK_DEV = 64
SECTIONS = 32
SOURCES = 32
GROUP = 4
FF_DEV = 256
SLICES = 32
EXPERTS = 8
TOKENS = 2048
CAPACITY = 8


def route_block(block_key):
    key_tokens, key_within, key_offset, key_relabel = jax.random.split(block_key, 4)
    token_order = jax.random.permutation(key_tokens, TOK_DEV)
    within_keys = jax.random.split(key_within, TOK_DEV)

    def shuffle_slots(single_key):
        return jax.random.permutation(single_key, TOP)
    within_token = jax.vmap(shuffle_slots)(within_keys)
    offset = jax.random.randint(key_offset, (), 0, EXPERTS)
    relabel = jax.random.permutation(key_relabel, EXPERTS)
    position = token_order[:, None] * TOP + within_token + offset
    return relabel[position % EXPERTS].astype(jnp.int32)


def route_table(key, salt):
    salted = jax.random.fold_in(key, salt)
    block_keys = jax.random.split(salted, SECTIONS * SOURCES)
    blocks = jax.vmap(route_block)(block_keys)
    return blocks.reshape(SECTIONS, TOKENS, TOP).astype(jnp.int32)


def draw_forward_ids(key, part):
    return route_table(key, 11)


def draw_grad_ids(key, part):
    return route_table(key, 23)


def shard_levels(stream_key, shape, cuts, least, largest):
    level, own = 1.0, jax.random.fold_in(stream_key, 6)
    for dim, shards_of in cuts:
        heights = jnp.exp(jax.random.uniform(jax.random.fold_in(own, dim), (shards_of,), jnp.float32, least / len(cuts), largest / len(cuts)))
        level = level * jnp.repeat(heights, shape[dim] // shards_of).reshape([-1 if axis == dim else 1 for axis in range(len(shape))])
    return level


def bell_draw(stream_key, dims, scale, most, cuts=(), dtype=jnp.bfloat16):
    level = shard_levels(stream_key, dims, cuts, -0.22, 0.18) if cuts else 1.0
    values = jax.random.normal(stream_key, dims, jnp.float32) * scale * level
    return jnp.minimum(jnp.maximum(values, -most), most).astype(dtype)


def setup_inputs(seed: int = 0) -> dict:
    arg_keys = jax.random.split(jax.random.key(seed), 12)
    return {
        "forward_in": bell_draw(arg_keys[0], (SECTIONS, TOKENS, D), 1.0, 6.0, ((0, 32), (1, 32))),
        "forward_ids": draw_forward_ids(jax.random.fold_in(arg_keys[11], 71), 0),
        "forward_gates": jnp.clip(0.4 + 0.6 * jax.random.uniform(arg_keys[2], (SECTIONS, TOKENS, TOP), jnp.float32) ** shard_levels(arg_keys[2], (SECTIONS, TOKENS, TOP), ((0, 32), (1, 32)), -0.2, 0.2), 0.4, 1.0),
        "grad_in": bell_draw(arg_keys[3], (SECTIONS, TOKENS, D), 1.0, 6.0, ((0, 32), (1, 32))),
        "grad_ids": draw_grad_ids(jax.random.fold_in(arg_keys[11], 71), 0),
        "grad_gates": jnp.clip(0.4 + 0.6 * jax.random.uniform(arg_keys[5], (SECTIONS, TOKENS, TOP), jnp.float32) ** shard_levels(arg_keys[5], (SECTIONS, TOKENS, TOP), ((0, 32), (1, 32)), -0.2, 0.2), 0.4, 1.0),
        "saved_input": bell_draw(arg_keys[6], (SECTIONS, TOKENS, D), 1.0, 6.0, ((0, 32), (1, 32))),
        "saved_acts": bell_draw(arg_keys[7], (SECTIONS, SLICES, SOURCES * CAPACITY, 2 * FF_DEV), 1.5, 8.0, ((0, 32), (1, 32))),
        "norm_gain": jnp.clip(1.0 + 0.18 * jax.random.normal(arg_keys[8], (SECTIONS, D), jnp.float32), 0.1, 1.9),
        "weight_in": bell_draw(arg_keys[9], (SLICES, D, 2 * FF_DEV), D ** -0.5, 0.09375, ((0, 32),)),
        "weight_out": bell_draw(arg_keys[10], (SLICES, FF_DEV, D), FFW ** -0.5, 0.1875, ((0, 32),)),
    }


epsilon = 1e-06

def normalize(tokens, norm_scale):
    widened = tokens.astype(jnp.float32)
    inverse_rms = lax.rsqrt(lax.optimization_barrier(jnp.mean(widened * widened, axis=-1, keepdims=True)) + epsilon)
    return (widened * inverse_rms * norm_scale).astype(jnp.bfloat16)

def slot_order(route_ids):
    flattened = route_ids.reshape(-1)
    sorted_pairs = jnp.argsort(flattened, stable=True).astype(jnp.int32)
    inverse_pairs = jnp.argsort(sorted_pairs, stable=True).astype(jnp.int32)
    return (sorted_pairs, inverse_pairs)

def reference(forward_in, forward_ids, forward_gates, grad_in, grad_ids, grad_gates, saved_input, saved_acts, norm_gain, weight_in, weight_out):
    w_first = weight_in.astype(jnp.float32).reshape(EXPERTS, GROUP, D, 2 * FF_DEV)
    w_second = weight_out.astype(jnp.float32).reshape(EXPERTS, GROUP, FF_DEV, D)

    def section_forward(operands):
        tokens, route_ids, gate_values, norm_scale = operands
        normed = normalize(tokens, norm_scale)
        sorted_pairs, inverse_pairs = slot_order(route_ids)
        grouped = jnp.take(normed, sorted_pairs // TOP, axis=0).reshape(EXPERTS, -1, D).astype(jnp.float32)
        projected = jnp.einsum('erd,egdf->egrf', grouped, w_first)
        hidden = (jax.nn.silu(projected[..., :FF_DEV]) * projected[..., FF_DEV:]).astype(jnp.bfloat16)
        parts = jnp.einsum('egrf,egfd->egrd', hidden.astype(jnp.float32), w_second).astype(jnp.bfloat16)
        pair_out = lax.optimization_barrier(jnp.sum(parts.astype(jnp.float32), axis=1)).reshape(-1, D)
        paired = jnp.take(pair_out, inverse_pairs, axis=0).reshape(-1, TOP, D)
        combined = jnp.einsum('tk,tkd->td', gate_values, paired)
        return (tokens.astype(jnp.float32) + combined).astype(jnp.bfloat16)

    def section_backward(operands):
        grads, route_ids, gate_values, before, stored, norm_scale = operands
        sorted_pairs, inverse_pairs = slot_order(route_ids)
        grouped = jnp.take(grads, sorted_pairs // TOP, axis=0).reshape(EXPERTS, -1, D).astype(jnp.float32)
        stored_wide = stored.astype(jnp.float32).reshape(EXPERTS, GROUP, -1, 2 * FF_DEV)
        hidden_grad = jnp.einsum('erd,egfd->egrf', grouped, w_second)
        gate_act = stored_wide[..., :FF_DEV]
        up_act = stored_wide[..., FF_DEV:]
        squashed = jax.nn.sigmoid(gate_act)
        gate_grad = (hidden_grad * up_act * squashed * (1.0 + gate_act * (1.0 - squashed))).astype(jnp.bfloat16)
        up_grad = (hidden_grad * gate_act * squashed).astype(jnp.bfloat16)
        joined = jnp.concatenate([gate_grad, up_grad], axis=-1).astype(jnp.float32)
        parts = jnp.einsum('egrf,egdf->egrd', joined, w_first).astype(jnp.bfloat16)
        pair_back = lax.optimization_barrier(jnp.sum(parts.astype(jnp.float32), axis=1)).reshape(-1, D)
        paired = jnp.take(pair_back, inverse_pairs, axis=0).reshape(-1, TOP, D)
        pulled = jnp.einsum('tk,tkd->td', gate_values, paired)
        widened = before.astype(jnp.float32)
        inverse_rms = lax.rsqrt(lax.optimization_barrier(jnp.mean(widened * widened, axis=-1, keepdims=True)) + epsilon)
        unit_rows = widened * inverse_rms
        weighted = pulled * norm_scale
        through = grads.astype(jnp.float32) + inverse_rms * (weighted - unit_rows * lax.optimization_barrier(jnp.mean(weighted * unit_rows, axis=-1, keepdims=True)))
        return through.astype(jnp.bfloat16)
    moved = lax.map(section_forward, (forward_in, forward_ids, forward_gates, norm_gain))
    through = lax.map(section_backward, (grad_in, grad_ids, grad_gates, saved_input, saved_acts, norm_gain))
    return (jnp.roll(moved, 1, axis=0), jnp.roll(through, -1, axis=0))
```

```python
import jax
import jax.numpy as jnp
from jax import lax
from jax.sharding import Mesh, PartitionSpec as P

epsilon = 1e-06
PLANE = ("x", "y", "c")
RING = ("zh", "zl")


def normalize(tokens, norm_scale):
    widened = tokens.astype(jnp.float32)
    inverse_rms = lax.rsqrt(jnp.mean(widened * widened, axis=-1, keepdims=True) + epsilon)
    return (widened * inverse_rms * norm_scale).astype(jnp.bfloat16)


def slot_order(route_ids):
    flattened = route_ids.reshape(-1)
    sorted_pairs = jnp.argsort(flattened, stable=True)
    inverse_pairs = jnp.argsort(sorted_pairs, stable=True)
    return (sorted_pairs, inverse_pairs)


def swapped(parts):
    parts = lax.all_to_all(parts, "zh", split_axis=0, concat_axis=0, tiled=True)
    return lax.all_to_all(parts, "x", split_axis=0, concat_axis=0, tiled=True)


def moved_weight(weight):
    rows, columns = weight.shape
    blocks, run, across = lax.axis_size("zh"), lax.axis_size("zl"), lax.axis_size("x")
    height, width = rows // (blocks * run), columns // across
    cut = weight.reshape(blocks, run, height, columns)
    mine = lax.dynamic_slice(
        cut,
        (0, lax.axis_index("zl"), 0, lax.axis_index("x") * width),
        (blocks, 1, height, width),
    )[:, 0]
    strips = swapped(mine)
    part = strips.transpose(1, 0, 2).reshape(height, columns)
    return lax.all_gather(part, RING, axis=0, tiled=True)


def deliver(grouped):
    experts, capacity, width = grouped.shape
    ys, cs = lax.axis_size("y"), lax.axis_size("c")
    pairs = experts // ys
    half = lax.axis_size("x") // pairs
    by_place = grouped.reshape(ys, pairs, capacity, width).transpose(1, 0, 2, 3)
    outgoing = jnp.broadcast_to(
        by_place[:, None, :, None], (pairs, half, ys, cs, capacity, width)
    ).reshape(pairs * half * ys * cs, capacity, width)
    return lax.all_to_all(outgoing, PLANE, split_axis=0, concat_axis=0, tiled=True)


def collect(partial_rows, experts):
    slices, capacity, width = partial_rows.shape
    ys, cs = lax.axis_size("y"), lax.axis_size("c")
    pairs = experts // ys
    half = lax.axis_size("x") // pairs
    arrived = lax.all_to_all(partial_rows, PLANE, split_axis=0, concat_axis=0, tiled=True)
    summed = jnp.sum(
        arrived.reshape(pairs, half, ys, cs, capacity, width).astype(jnp.float32), axis=(1, 3)
    )
    return summed.transpose(1, 0, 2, 3).reshape(experts * capacity, width)


def shifted(array, by):
    sections = lax.axis_size(("x", "zl"))
    return lax.ppermute(array, ("x", "zl"), [(i, (i + by) % sections) for i in range(sections)])


def on_device(
    forward_in,
    forward_ids,
    forward_gates,
    grad_in,
    grad_ids,
    grad_gates,
    saved_input,
    saved_acts,
    norm_gain,
    weight_in,
    weight_out,
):
    tokens = forward_in[0]
    sources = lax.axis_size(("y", "zh", "c"))
    token_count, top_count = forward_ids[0].shape
    model_width = tokens.shape[1]
    group_size = min(4, sources // 2)
    expert_count = sources // group_size
    capacity = token_count * top_count // expert_count
    norm_scale = norm_gain[0]
    hidden_width = weight_out.shape[1]

    w_first = moved_weight(weight_in[0])
    w_second = moved_weight(weight_out[0])
    ys, blocks, cs = lax.axis_size("y"), lax.axis_size("zh"), lax.axis_size("c")
    acts = saved_acts[0, 0].reshape(ys, blocks, cs * capacity, 2 * hidden_width)
    acts = acts.transpose(1, 0, 2, 3).reshape(blocks, ys * cs * capacity, 2 * hidden_width)
    stored = swapped(acts).reshape(-1, capacity, 2 * hidden_width)

    normed = normalize(tokens, norm_scale)
    fwd_sorted, fwd_inverse = slot_order(forward_ids[0])
    grad_sorted, grad_inverse = slot_order(grad_ids[0])
    fwd_grouped = jnp.take(normed, fwd_sorted // top_count, axis=0).reshape(
        expert_count, capacity, model_width
    )
    grad_grouped = jnp.take(grad_in[0], grad_sorted // top_count, axis=0).reshape(
        expert_count, capacity, model_width
    )
    fwd_arrived = deliver(fwd_grouped)
    grad_arrived = deliver(grad_grouped)

    projected = jnp.einsum("scd,df->scf", fwd_arrived, w_first, preferred_element_type=jnp.float32)
    hidden = (jax.nn.silu(projected[..., :hidden_width]) * projected[..., hidden_width:]).astype(
        jnp.bfloat16
    )
    fwd_partial = jnp.einsum(
        "scf,fd->scd", hidden, w_second, preferred_element_type=jnp.float32
    ).astype(jnp.bfloat16)
    fwd_flat = collect(fwd_partial, expert_count)

    hidden_grad = jnp.einsum(
        "scd,fd->scf", grad_arrived, w_second, preferred_element_type=jnp.float32
    )
    gate_act = stored[..., :hidden_width].astype(jnp.float32)
    up_act = stored[..., hidden_width:].astype(jnp.float32)
    squashed = jax.nn.sigmoid(gate_act)
    gate_grad = (hidden_grad * up_act * squashed * (1.0 + gate_act * (1.0 - squashed))).astype(
        jnp.bfloat16
    )
    up_grad = (hidden_grad * gate_act * squashed).astype(jnp.bfloat16)
    joined = jnp.concatenate([gate_grad, up_grad], axis=-1)
    grad_partial = jnp.einsum(
        "scf,df->scd", joined, w_first, preferred_element_type=jnp.float32
    ).astype(jnp.bfloat16)
    grad_flat = collect(grad_partial, expert_count)

    fwd_pairs = jnp.take(fwd_flat, fwd_inverse, axis=0).reshape(token_count, top_count, model_width)
    combined = jnp.einsum("tk,tkd->td", forward_gates[0], fwd_pairs)
    moved = (tokens.astype(jnp.float32) + combined).astype(jnp.bfloat16)
    grad_pairs = jnp.take(grad_flat, grad_inverse, axis=0).reshape(
        token_count, top_count, model_width
    )
    pulled = jnp.einsum("tk,tkd->td", grad_gates[0], grad_pairs)
    widened = saved_input[0].astype(jnp.float32)
    inverse_rms = lax.rsqrt(jnp.mean(widened * widened, axis=-1, keepdims=True) + epsilon)
    unit_rows = widened * inverse_rms
    weighted = pulled * norm_scale
    through = grad_in[0].astype(jnp.float32) + inverse_rms * (
        weighted - unit_rows * jnp.mean(weighted * unit_rows, axis=-1, keepdims=True)
    )
    through = through.astype(jnp.bfloat16)
    return (shifted(moved[None], 1), shifted(through[None], -1))


def solution(mesh):
    fine = Mesh(mesh.devices.reshape(4, -1, 4, 4, 2), ("x", "zl", "y", "zh", "c"))
    pipe, expert = ("x", "zl"), ("y", "zh", "c")
    rows = P(pipe, expert, None)
    placed = (rows,) * 7 + (
        P(pipe, expert, None, None),
        P(pipe, None),
        P(expert, None, None),
        P(expert, None, None),
    )
    return jax.shard_map(
        on_device, mesh=fine, in_specs=placed, out_specs=(rows, rows), check_vma=False
    )
```

```python
import jax
import jax.numpy as jnp
import numpy as np
from jax import lax
from jax.experimental import pallas as pl
from jax.experimental.pallas import tpu as pltpu
from jax.sharding import Mesh, PartitionSpec as P

epsilon = 1e-06
PIPE = ("x", "zj", "zp")
FAR = ("zh", "c")
NEAR = ("x", "zp")
GROUP = ("x", "zp", "y")
RING = ("zh", "zj", "c")


def normalize(tokens, norm_scale):
    widened = tokens.astype(jnp.float32)
    inverse_rms = lax.rsqrt(jnp.mean(widened * widened, axis=-1, keepdims=True) + epsilon)
    return (widened * inverse_rms * norm_scale).astype(jnp.bfloat16)


def selection(route_ids, experts, capacity):
    ids = route_ids[:, 0]
    tokens = ids.shape[0]
    row = lax.broadcasted_iota(jnp.int32, (tokens, tokens), 0)
    column = lax.broadcasted_iota(jnp.int32, (tokens, tokens), 1)
    earlier = (ids[:, None] == ids[None, :]) & (column < row)
    slot = ids * capacity + jnp.sum(earlier.astype(jnp.int32), axis=1)
    xs, zs, ys = lax.axis_size("x"), lax.axis_size("zp"), lax.axis_size("y")
    pairs = experts // ys
    x, _, y, rank = np.indices((xs, zs, ys, capacity))
    place = ((y * pairs + x // (xs // pairs)) * capacity + rank).reshape(1, -1)
    return (slot[:, None] == jnp.asarray(place, jnp.int32)).astype(jnp.bfloat16)


def exchanged(rows, axes):
    return lax.all_to_all(rows, axes, split_axis=0, concat_axis=0, tiled=True)


def weight_pieces(weight_in, weight_out):
    width, columns = weight_in.shape
    hidden = weight_out.shape[0]
    far, run, parts = lax.axis_size(FAR), lax.axis_size("zj"), lax.axis_size(RING)
    zh, cs = lax.axis_size("zh"), lax.axis_size("c")
    strips, halves = lax.axis_size("x"), lax.axis_size("zp")
    tall, wide = width // parts // halves, columns // strips
    deep = hidden // parts
    pieces = width // columns
    j, x, half = lax.axis_index("zj"), lax.axis_index("x"), lax.axis_index("zp")
    first = lax.dynamic_slice(
        weight_in.reshape(zh, run, cs, halves, tall, columns),
        (0, j, 0, half, 0, x * wide),
        (zh, 1, cs, 1, tall, wide),
    ).reshape(far, tall, wide)
    piece = jnp.minimum(x * halves + half, pieces - 1)
    second = lax.dynamic_slice(
        weight_out.reshape(zh, run, cs, deep, width),
        (0, j, 0, 0, piece * columns),
        (zh, 1, cs, deep, columns),
    )
    second = second.reshape(far, deep, strips, wide).transpose(0, 2, 1, 3)
    return jnp.concatenate([first, second.reshape(far, strips * deep, wide)], axis=1)


def expert_kernel(fwd_ref, grad_ref, acts_ref, parts_ref, fwd_out, grad_out, first_ref, second_ref, sems):
    parts, halves, tall, columns = first_ref.shape
    _, deep, width = second_ref.shape
    wide = parts_ref.shape[3]
    strips = columns // wide
    hidden = parts * deep
    first_copies = [
        pltpu.make_async_copy(
            parts_ref.at[:, s * halves + h, pl.ds(0, tall), :],
            first_ref.at[:, h, :, pl.ds(s * wide, wide)],
            sems.at[s * halves + h],
        )
        for s in range(strips)
        for h in range(halves)
    ]
    second_copies = [
        pltpu.make_async_copy(
            parts_ref.at[:, q // strips, pl.ds(tall + q % strips * deep, deep), :],
            second_ref.at[:, :, pl.ds(q * wide, wide)],
            sems.at[strips * halves + q],
        )
        for q in range(width // wide)
    ]
    for copy in first_copies + second_copies:
        copy.start()
    for copy in first_copies:
        copy.wait()
    first = first_ref[...].reshape(parts * halves * tall, columns)
    projected = jnp.dot(fwd_ref[...], first, preferred_element_type=jnp.float32)
    gate, up = projected[:, :hidden], projected[:, hidden:]
    mixed = (gate / (1.0 + jnp.exp(-gate)) * up).astype(jnp.bfloat16)
    for copy in second_copies:
        copy.wait()
    second = second_ref[...].reshape(hidden, width)
    fwd_out[...] = jnp.dot(mixed, second, preferred_element_type=jnp.float32).astype(jnp.bfloat16)
    turned = (((1,), (1,)), ((), ()))
    hidden_grad = lax.dot_general(grad_ref[...], second, turned, preferred_element_type=jnp.float32)
    gate_act = acts_ref[:, :hidden].astype(jnp.float32)
    up_act = acts_ref[:, hidden:].astype(jnp.float32)
    squashed = 1.0 / (1.0 + jnp.exp(-gate_act))
    gate_grad = hidden_grad * up_act * squashed * (1.0 + gate_act * (1.0 - squashed))
    up_grad = hidden_grad * gate_act * squashed
    joined = jnp.concatenate([gate_grad.astype(jnp.bfloat16), up_grad.astype(jnp.bfloat16)], axis=1)
    grad_out[...] = lax.dot_general(
        joined, first, turned, preferred_element_type=jnp.float32
    ).astype(jnp.bfloat16)


def experts_of(fwd_rows, grad_rows, acts, parts, halves, deep):
    count, pieces, height, wide = parts.shape
    rows, width = fwd_rows.shape
    columns = acts.shape[1]
    tall = width // count // halves
    vmem, hbm = pl.BlockSpec(memory_space=pltpu.VMEM), pl.BlockSpec(memory_space=pl.ANY)
    out = jax.ShapeDtypeStruct((rows, width), jnp.bfloat16)
    return pl.pallas_call(
        expert_kernel,
        out_shape=(out, out),
        in_specs=[vmem, vmem, vmem, hbm],
        out_specs=(vmem, vmem),
        scratch_shapes=[
            pltpu.VMEM((count, halves, tall, columns), jnp.bfloat16),
            pltpu.VMEM((count, deep, width), jnp.bfloat16),
            pltpu.SemaphoreType.DMA((pieces + width // wide,)),
        ],
        compiler_params=pltpu.CompilerParams(vmem_limit_bytes=40 * 1024 * 1024),
        cost_estimate=pl.CostEstimate(
            flops=12 * rows * width * count * deep,
            bytes_accessed=count * pieces * height * wide * 2,
            transcendentals=2 * rows * count * deep,
        ),
        name="experts",
    )(fwd_rows, grad_rows, acts, parts)


def shifted(array, by):
    sections = lax.axis_size(PIPE)
    return lax.ppermute(array, PIPE, [(i, (i + by) % sections) for i in range(sections)])


def picked(chosen, rows, axis):
    return lax.dot_general(
        chosen, rows, (((axis,), (0,)), ((), ())), preferred_element_type=jnp.float32
    )


def on_device(
    forward_in,
    forward_ids,
    forward_gates,
    grad_in,
    grad_ids,
    grad_gates,
    saved_input,
    saved_acts,
    norm_gain,
    weight_in,
    weight_out,
):
    tokens, grads, norm_scale = forward_in[0], grad_in[0], norm_gain[0]
    token_count, model_width = tokens.shape
    experts = lax.axis_size(("y", "zh", "c")) // 4
    capacity = token_count // experts
    hidden, columns = weight_out.shape[1], weight_in.shape[2]
    places = lax.axis_size(GROUP)

    got = exchanged(weight_pieces(weight_in[0], weight_out[0]), FAR)
    grad_chosen = selection(grad_ids[0], experts, capacity)
    grad_sent = picked(grad_chosen, grads, 0).astype(jnp.bfloat16)
    grad_rows = exchanged(grad_sent.reshape(places, capacity, model_width), GROUP)
    part = exchanged(got, NEAR)
    parts = lax.all_gather(part, RING, axis=0)

    fwd_chosen = selection(forward_ids[0], experts, capacity)
    fwd_sent = picked(fwd_chosen, normalize(tokens, norm_scale), 0).astype(jnp.bfloat16)
    fwd_rows = exchanged(fwd_sent.reshape(places, capacity, model_width), GROUP)
    ys, far = lax.axis_size("y"), lax.axis_size(FAR)
    acts = saved_acts[0, 0].reshape(ys, far, capacity, columns).transpose(1, 0, 2, 3)
    acts = exchanged(acts.reshape(far, ys * capacity, columns), FAR)
    acts = exchanged(acts, NEAR)

    rows = places * capacity
    fwd_part, grad_part = experts_of(
        fwd_rows.reshape(rows, model_width),
        grad_rows.reshape(rows, model_width),
        acts.reshape(rows, columns),
        parts,
        lax.axis_size("zp"),
        hidden // lax.axis_size(RING),
    )
    fwd_back = exchanged(fwd_part.reshape(places, capacity, model_width), GROUP)
    grad_back = exchanged(grad_part.reshape(places, capacity, model_width), GROUP)

    combined = forward_gates[0] * picked(fwd_chosen, fwd_back.reshape(rows, model_width), 1)
    moved = (tokens.astype(jnp.float32) + combined).astype(jnp.bfloat16)
    pulled = grad_gates[0] * picked(grad_chosen, grad_back.reshape(rows, model_width), 1)
    widened = saved_input[0].astype(jnp.float32)
    inverse_rms = lax.rsqrt(jnp.mean(widened * widened, axis=-1, keepdims=True) + epsilon)
    unit_rows = widened * inverse_rms
    weighted = pulled * norm_scale
    through = grads.astype(jnp.float32) + inverse_rms * (
        weighted - unit_rows * jnp.mean(weighted * unit_rows, axis=-1, keepdims=True)
    )
    return (shifted(moved[None], 1), shifted(through.astype(jnp.bfloat16)[None], -1))


def solution(mesh):
    fine = Mesh(mesh.devices.reshape(4, 4, 2, 4, 4, 2), ("x", "zj", "zp", "y", "zh", "c"))
    expert = ("y", "zh", "c")
    rows = P(PIPE, expert, None)
    placed = (rows,) * 7 + (
        P(PIPE, expert, None, None),
        P(PIPE, None),
        P(expert, None, None),
        P(expert, None, None),
    )
    return jax.shard_map(
        on_device, mesh=fine, in_specs=placed, out_specs=(rows, rows), check_vma=False
    )
```

```python
import jax
import jax.numpy as jnp
import numpy as np
from jax import lax
from jax.experimental import pallas as pl
from jax.experimental.pallas import tpu as pltpu
from jax.sharding import Mesh, PartitionSpec as P

epsilon = 1e-06
PIPE = ("x", "zj", "zp")
FAR = ("zh", "c")
NEAR = ("x", "zp")
PLANE = ("x", "y")
BACK = ("x", "y", "zp")
RING = ("zh", "zj", "c")


def normalize(tokens, norm_scale):
    widened = tokens.astype(jnp.float32)
    inverse_rms = lax.rsqrt(jnp.mean(widened * widened, axis=-1, keepdims=True) + epsilon)
    return (widened * inverse_rms * norm_scale).astype(jnp.bfloat16)


def slots(route_ids, capacity):
    ids = route_ids[:, 0]
    tokens = ids.shape[0]
    row = lax.broadcasted_iota(jnp.int32, (tokens, tokens), 0)
    column = lax.broadcasted_iota(jnp.int32, (tokens, tokens), 1)
    earlier = (ids[:, None] == ids[None, :]) & (column < row)
    return ids * capacity + jnp.sum(earlier.astype(jnp.int32), axis=1)


def grouped(slot, rows):
    chosen = slot[:, None] == lax.broadcasted_iota(jnp.int32, (rows.shape[0],) * 2, 1)
    return picked(chosen.astype(jnp.bfloat16), rows, 0).astype(jnp.bfloat16)


def returned(slot, rows, experts, capacity):
    xs, ys, zs = lax.axis_size("x"), lax.axis_size("y"), lax.axis_size("zp")
    pairs = experts // ys
    x, y, _, rank = np.indices((xs, ys, zs, capacity))
    place = ((y * pairs + x // (xs // pairs)) * capacity + rank).reshape(1, -1)
    chosen = slot[:, None] == jnp.asarray(place, jnp.int32)
    return picked(chosen.astype(jnp.bfloat16), rows, 1)


def swapped_rows(rows):
    zs = lax.axis_size("zp")
    return lax.ppermute(rows, "zp", [(i, zs - 1 - i) for i in range(zs)])


def for_plane(own, partner, experts, capacity):
    xs, ys, zs = lax.axis_size("x"), lax.axis_size("y"), lax.axis_size("zp")
    pairs = experts // ys
    width = own.shape[1]
    even = lax.axis_index("zp") == 0
    both = jnp.stack([jnp.where(even, own, partner), jnp.where(even, partner, own)])
    both = both.reshape(zs, ys, pairs, capacity, width).transpose(2, 1, 0, 3, 4)
    both = jnp.broadcast_to(both[:, None], (pairs, xs // pairs, ys, zs, capacity, width))
    return both.reshape(xs * ys, zs * capacity, width)


def exchanged(rows, axes):
    return lax.all_to_all(rows, axes, split_axis=0, concat_axis=0, tiled=True)


def weight_pieces(weight_in, weight_out):
    width, columns = weight_in.shape
    hidden = weight_out.shape[0]
    far, run, parts = lax.axis_size(FAR), lax.axis_size("zj"), lax.axis_size(RING)
    zh, cs = lax.axis_size("zh"), lax.axis_size("c")
    strips, halves = lax.axis_size("x"), lax.axis_size("zp")
    tall, wide = width // parts // halves, columns // strips
    deep = hidden // parts
    pieces = width // columns
    j, x, half = lax.axis_index("zj"), lax.axis_index("x"), lax.axis_index("zp")
    first = lax.dynamic_slice(
        weight_in.reshape(zh, run, cs, halves, tall, columns),
        (0, j, 0, half, 0, x * wide),
        (zh, 1, cs, 1, tall, wide),
    ).reshape(far, tall, wide)
    piece = jnp.minimum(x * halves + half, pieces - 1)
    second = lax.dynamic_slice(
        weight_out.reshape(zh, run, cs, deep, width),
        (0, j, 0, 0, piece * columns),
        (zh, 1, cs, deep, columns),
    )
    second = second.reshape(far, deep, strips, wide).transpose(0, 2, 1, 3)
    return jnp.concatenate([first, second.reshape(far, strips * deep, wide)], axis=1)


def weight_copies(parts_ref, first_ref, second_ref, sems):
    _, halves, tall, columns = first_ref.shape
    _, deep, width = second_ref.shape
    wide = parts_ref.shape[3]
    strips = columns // wide
    first_copies = [
        pltpu.make_async_copy(
            parts_ref.at[:, s * halves + h, pl.ds(0, tall), :],
            first_ref.at[:, h, :, pl.ds(s * wide, wide)],
            sems.at[1 + s * halves + h],
        )
        for s in range(strips)
        for h in range(halves)
    ]
    second_copies = [
        pltpu.make_async_copy(
            parts_ref.at[:, q // strips, pl.ds(tall + q % strips * deep, deep), :],
            second_ref.at[:, :, pl.ds(q * wide, wide)],
            sems.at[1 + strips * halves + q],
        )
        for q in range(width // wide)
    ]
    return first_copies, second_copies


def forward_kernel(rows_hbm, parts_ref, out_ref, rows_ref, first_ref, second_ref, sems):
    parts, halves, tall, columns = first_ref.shape
    _, deep, width = second_ref.shape
    hidden = parts * deep
    first_copies, second_copies = weight_copies(parts_ref, first_ref, second_ref, sems)
    rows_copy = pltpu.make_async_copy(rows_hbm, rows_ref, sems.at[0])
    for copy in [rows_copy] + first_copies + second_copies:
        copy.start()
    for copy in [rows_copy] + first_copies:
        copy.wait()
    first = first_ref[...].reshape(parts * halves * tall, columns)
    projected = jnp.dot(rows_ref[...], first, preferred_element_type=jnp.float32)
    gate, up = projected[:, :hidden], projected[:, hidden:]
    mixed = (gate / (1.0 + jnp.exp(-gate)) * up).astype(jnp.bfloat16)
    for copy in second_copies:
        copy.wait()
    second = second_ref[...].reshape(hidden, width)
    out_ref[...] = jnp.dot(mixed, second, preferred_element_type=jnp.float32).astype(jnp.bfloat16)


def gradient_kernel(rows_hbm, parts_ref, acts_ref, out_ref, rows_ref, first_ref, second_ref, sems):
    parts, halves, tall, columns = first_ref.shape
    _, deep, width = second_ref.shape
    hidden = parts * deep
    first_copies, second_copies = weight_copies(parts_ref, first_ref, second_ref, sems)
    rows_copy = pltpu.make_async_copy(rows_hbm, rows_ref, sems.at[0])
    for copy in [rows_copy] + second_copies + first_copies:
        copy.start()
    for copy in [rows_copy] + second_copies:
        copy.wait()
    turned = (((1,), (1,)), ((), ()))
    second = second_ref[...].reshape(hidden, width)
    hidden_grad = lax.dot_general(rows_ref[...], second, turned, preferred_element_type=jnp.float32)
    gate_act = acts_ref[:, :hidden].astype(jnp.float32)
    up_act = acts_ref[:, hidden:].astype(jnp.float32)
    squashed = 1.0 / (1.0 + jnp.exp(-gate_act))
    gate_grad = hidden_grad * up_act * squashed * (1.0 + gate_act * (1.0 - squashed))
    up_grad = hidden_grad * gate_act * squashed
    joined = jnp.concatenate([gate_grad.astype(jnp.bfloat16), up_grad.astype(jnp.bfloat16)], axis=1)
    for copy in first_copies:
        copy.wait()
    first = first_ref[...].reshape(parts * halves * tall, columns)
    out_ref[...] = lax.dot_general(
        joined, first, turned, preferred_element_type=jnp.float32
    ).astype(jnp.bfloat16)


def experts_of(kernel, rows, parts, halves, hidden, *more):
    count, pieces, height, wide = parts.shape
    height_rows, width = rows.shape
    columns = 2 * hidden
    deep, tall = hidden // count, width // count // halves
    vmem, hbm = pl.BlockSpec(memory_space=pltpu.VMEM), pl.BlockSpec(memory_space=pl.ANY)
    return pl.pallas_call(
        kernel,
        out_shape=jax.ShapeDtypeStruct((height_rows, width), jnp.bfloat16),
        in_specs=[hbm, hbm] + [vmem] * len(more),
        out_specs=vmem,
        scratch_shapes=[
            pltpu.VMEM((height_rows, width), jnp.bfloat16),
            pltpu.VMEM((count, halves, tall, columns), jnp.bfloat16),
            pltpu.VMEM((count, deep, width), jnp.bfloat16),
            pltpu.SemaphoreType.DMA((1 + pieces + width // wide,)),
        ],
        compiler_params=pltpu.CompilerParams(vmem_limit_bytes=32 * 1024 * 1024),
        cost_estimate=pl.CostEstimate(
            flops=6 * height_rows * width * hidden,
            bytes_accessed=count * pieces * height * wide * 2,
            transcendentals=height_rows * hidden,
        ),
    )(rows, parts, *more)


def shifted(array, by):
    sections = lax.axis_size(PIPE)
    return lax.ppermute(array, PIPE, [(i, (i + by) % sections) for i in range(sections)])


def picked(chosen, rows, axis):
    return lax.dot_general(
        chosen, rows, (((axis,), (0,)), ((), ())), preferred_element_type=jnp.float32
    )


def on_device(
    forward_in,
    forward_ids,
    forward_gates,
    grad_in,
    grad_ids,
    grad_gates,
    saved_input,
    saved_acts,
    norm_gain,
    weight_in,
    weight_out,
):
    grads, norm_scale = grad_in[0], norm_gain[0]
    token_count, model_width = grads.shape
    experts = lax.axis_size(("y", "zh", "c")) // 4
    capacity = token_count // experts
    hidden, columns = weight_out.shape[1], weight_in.shape[2]
    halves, places = lax.axis_size("zp"), lax.axis_size(BACK)
    rows = places * capacity

    got = exchanged(weight_pieces(weight_in[0], weight_out[0]), FAR)
    part = exchanged(got, NEAR)
    parts = lax.all_gather(part, RING, axis=0)

    grad_slot = slots(grad_ids[0], capacity)
    grad_own = grouped(grad_slot, grads)
    grad_partner = swapped_rows(grad_own)

    small = jnp.concatenate(
        [norm_scale, forward_ids[0, :, 0].astype(jnp.float32), forward_gates[0, :, 0]]
    )
    tokens = shifted(forward_in, 1)[0]
    small = shifted(small[None], 1)[0]
    fwd_scale = small[:model_width]
    fwd_ids = small[model_width : model_width + token_count].astype(jnp.int32)
    fwd_gates = small[model_width + token_count :]
    fwd_slot = slots(fwd_ids[:, None], capacity)
    fwd_own = grouped(fwd_slot, normalize(tokens, fwd_scale))
    fwd_partner = swapped_rows(fwd_own)

    xs, zs, ys, far = lax.axis_size("x"), lax.axis_size("zp"), lax.axis_size("y"), lax.axis_size(FAR)
    acts = saved_acts[0, 0].reshape(ys, far, capacity, columns).transpose(1, 0, 2, 3)
    acts = exchanged(acts.reshape(far, ys * capacity, columns), FAR)
    acts = exchanged(acts, NEAR)
    acts = acts.reshape(xs, zs, ys, capacity, columns).transpose(0, 2, 1, 3, 4)

    grad_sent = for_plane(grad_own, grad_partner, experts, capacity)
    grad_rows = exchanged(grad_sent, PLANE).reshape(rows, model_width)
    fwd_sent = for_plane(fwd_own, fwd_partner, experts, capacity)
    fwd_rows = exchanged(fwd_sent, PLANE).reshape(rows, model_width)

    grad_part = experts_of(
        gradient_kernel, grad_rows, parts, halves, hidden, acts.reshape(rows, columns)
    )
    grad_back = exchanged(grad_part.reshape(places, capacity, model_width), BACK)
    fwd_part = experts_of(forward_kernel, fwd_rows, parts, halves, hidden)
    fwd_back = exchanged(fwd_part.reshape(places, capacity, model_width), BACK)

    pulled = grad_gates[0] * returned(
        grad_slot, grad_back.reshape(rows, model_width), experts, capacity
    )
    widened = saved_input[0].astype(jnp.float32)
    inverse_rms = lax.rsqrt(jnp.mean(widened * widened, axis=-1, keepdims=True) + epsilon)
    unit_rows = widened * inverse_rms
    weighted = pulled * norm_scale
    through = grads.astype(jnp.float32) + inverse_rms * (
        weighted - unit_rows * jnp.mean(weighted * unit_rows, axis=-1, keepdims=True)
    )
    grad_out = shifted(through.astype(jnp.bfloat16)[None], -1)
    combined = fwd_gates[:, None] * returned(
        fwd_slot, fwd_back.reshape(rows, model_width), experts, capacity
    )
    moved = (tokens.astype(jnp.float32) + combined).astype(jnp.bfloat16)
    return (moved[None], grad_out)


def solution(mesh):
    fine = Mesh(mesh.devices.reshape(4, 4, 2, 4, 4, 2), ("x", "zj", "zp", "y", "zh", "c"))
    expert = ("y", "zh", "c")
    rows = P(PIPE, expert, None)
    placed = (rows,) * 7 + (
        P(PIPE, expert, None, None),
        P(PIPE, None),
        P(expert, None, None),
        P(expert, None, None),
    )
    return jax.shard_map(
        on_device, mesh=fine, in_specs=placed, out_specs=(rows, rows), check_vma=False
    )
```

```python
import jax
import jax.numpy as jnp
import numpy as np
from jax import lax
from jax.experimental import pallas as pl
from jax.experimental.pallas import tpu as pltpu
from jax.sharding import Mesh, PartitionSpec as P

epsilon = 1e-06
PIPE = ("x", "zj", "zp")
FAR = ("zh", "c")
NEAR = ("x", "zp")
PLANE = ("x", "y")
BACK = ("x", "y", "zp")
RING = ("zh", "zj", "c")


def normalize(tokens, norm_scale):
    widened = tokens.astype(jnp.float32)
    inverse_rms = lax.rsqrt(jnp.mean(widened * widened, axis=-1, keepdims=True) + epsilon)
    return (widened * inverse_rms * norm_scale).astype(jnp.bfloat16)


def slots(route_ids, capacity):
    ids = route_ids[:, 0]
    tokens = ids.shape[0]
    row = lax.broadcasted_iota(jnp.int32, (tokens, tokens), 0)
    column = lax.broadcasted_iota(jnp.int32, (tokens, tokens), 1)
    earlier = (ids[:, None] == ids[None, :]) & (column < row)
    return ids * capacity + jnp.sum(earlier.astype(jnp.int32), axis=1)


def grouped(slot, rows):
    chosen = slot[:, None] == lax.broadcasted_iota(jnp.int32, (rows.shape[0],) * 2, 1)
    return picked(chosen.astype(jnp.bfloat16), rows, 0).astype(jnp.bfloat16)


def returned(slot, rows, experts, capacity):
    xs, ys, zs = lax.axis_size("x"), lax.axis_size("y"), lax.axis_size("zp")
    pairs = experts // ys
    x, y, _, rank = np.indices((xs, ys, zs, capacity))
    place = ((y * pairs + x // (xs // pairs)) * capacity + rank).reshape(1, -1)
    chosen = slot[:, None] == jnp.asarray(place, jnp.int32)
    return picked(chosen.astype(jnp.bfloat16), rows, 1)


def swapped_rows(rows):
    zs = lax.axis_size("zp")
    return lax.ppermute(rows, "zp", [(i, zs - 1 - i) for i in range(zs)])


def for_plane(own, partner, experts, capacity):
    xs, ys, zs = lax.axis_size("x"), lax.axis_size("y"), lax.axis_size("zp")
    pairs = experts // ys
    width = own.shape[1]
    even = lax.axis_index("zp") == 0
    both = jnp.stack([jnp.where(even, own, partner), jnp.where(even, partner, own)])
    both = both.reshape(zs, ys, pairs, capacity, width).transpose(2, 1, 0, 3, 4)
    both = jnp.broadcast_to(both[:, None], (pairs, xs // pairs, ys, zs, capacity, width))
    return both.reshape(xs * ys, zs * capacity, width)


def exchanged(rows, axes):
    return lax.all_to_all(rows, axes, split_axis=0, concat_axis=0, tiled=True)


def weight_pieces(weight_in, weight_out):
    width, columns = weight_in.shape
    hidden = weight_out.shape[0]
    far, run, parts = lax.axis_size(FAR), lax.axis_size("zj"), lax.axis_size(RING)
    zh, cs = lax.axis_size("zh"), lax.axis_size("c")
    strips, halves = lax.axis_size("x"), lax.axis_size("zp")
    tall, wide = width // parts // halves, columns // strips
    deep = hidden // parts
    pieces = width // columns
    j, x, half = lax.axis_index("zj"), lax.axis_index("x"), lax.axis_index("zp")
    first = lax.dynamic_slice(
        weight_in.reshape(zh, run, cs, halves, tall, columns),
        (0, j, 0, half, 0, x * wide),
        (zh, 1, cs, 1, tall, wide),
    ).reshape(far, tall, wide)
    piece = jnp.minimum(x * halves + half, pieces - 1)
    second = lax.dynamic_slice(
        weight_out.reshape(zh, run, cs, deep, width),
        (0, j, 0, 0, piece * columns),
        (zh, 1, cs, deep, columns),
    )
    second = second.reshape(far, deep, strips, wide).transpose(0, 2, 1, 3)
    return jnp.concatenate([first, second.reshape(far, strips * deep, wide)], axis=1)


def weight_copies(parts_ref, first_ref, second_ref, sems):
    _, halves, tall, columns = first_ref.shape
    _, deep, width = second_ref.shape
    wide = parts_ref.shape[3]
    strips = columns // wide
    first_copies = [
        pltpu.make_async_copy(
            parts_ref.at[:, s * halves + h, pl.ds(0, tall), :],
            first_ref.at[:, h, :, pl.ds(s * wide, wide)],
            sems.at[1 + s * halves + h],
        )
        for s in range(strips)
        for h in range(halves)
    ]
    second_copies = [
        pltpu.make_async_copy(
            parts_ref.at[:, q // strips, pl.ds(tall + q % strips * deep, deep), :],
            second_ref.at[:, :, pl.ds(q * wide, wide)],
            sems.at[1 + strips * halves + q],
        )
        for q in range(width // wide)
    ]
    return first_copies, second_copies


def written(strip, out_hbm, out_ref, done):
    width = out_ref.shape[1] // done.shape[0]
    copies = []
    for q in range(done.shape[0]):
        part = slice(q * width, (q + 1) * width)
        out_ref[:, part] = strip(part).astype(jnp.bfloat16)
        columns_of = pl.ds(q * width, width)
        copies.append(
            pltpu.make_async_copy(out_ref.at[:, columns_of], out_hbm.at[:, columns_of], done.at[q])
        )
        copies[-1].start()
    for copy in copies:
        copy.wait()


def forward_kernel(rows_hbm, parts_ref, out_hbm, rows_ref, out_ref, first_ref, second_ref, sems, done):
    parts, halves, tall, columns = first_ref.shape
    _, deep, _ = second_ref.shape
    hidden = parts * deep
    first_copies, second_copies = weight_copies(parts_ref, first_ref, second_ref, sems)
    rows_copy = pltpu.make_async_copy(rows_hbm, rows_ref, sems.at[0])
    for copy in [rows_copy] + first_copies + second_copies:
        copy.start()
    for copy in [rows_copy] + first_copies:
        copy.wait()
    first = first_ref[...].reshape(parts * halves * tall, columns)
    projected = jnp.dot(rows_ref[...], first, preferred_element_type=jnp.float32)
    gate, up = projected[:, :hidden], projected[:, hidden:]
    mixed = (gate / (1.0 + jnp.exp(-gate)) * up).astype(jnp.bfloat16)
    for copy in second_copies:
        copy.wait()

    def strip(columns_of):
        second = second_ref[:, :, columns_of].reshape(hidden, -1)
        return jnp.dot(mixed, second, preferred_element_type=jnp.float32)

    written(strip, out_hbm, out_ref, done)


def gradient_kernel(
    rows_hbm, parts_ref, acts_ref, out_hbm, rows_ref, out_ref, first_ref, second_ref, sems, done
):
    parts, _, _, columns = first_ref.shape
    _, deep, width = second_ref.shape
    hidden = parts * deep
    first_copies, second_copies = weight_copies(parts_ref, first_ref, second_ref, sems)
    rows_copy = pltpu.make_async_copy(rows_hbm, rows_ref, sems.at[0])
    for copy in [rows_copy] + second_copies + first_copies:
        copy.start()
    for copy in [rows_copy] + second_copies:
        copy.wait()
    turned = (((1,), (1,)), ((), ()))
    second = second_ref[...].reshape(hidden, width)
    hidden_grad = lax.dot_general(rows_ref[...], second, turned, preferred_element_type=jnp.float32)
    gate_act = acts_ref[:, :hidden].astype(jnp.float32)
    up_act = acts_ref[:, hidden:].astype(jnp.float32)
    squashed = 1.0 / (1.0 + jnp.exp(-gate_act))
    gate_grad = hidden_grad * up_act * squashed * (1.0 + gate_act * (1.0 - squashed))
    up_grad = hidden_grad * gate_act * squashed
    joined = jnp.concatenate([gate_grad.astype(jnp.bfloat16), up_grad.astype(jnp.bfloat16)], axis=1)
    for copy in first_copies:
        copy.wait()

    first = first_ref[...].reshape(width, columns)

    def strip(columns_of):
        return lax.dot_general(
            joined, first[columns_of, :], turned, preferred_element_type=jnp.float32
        )

    written(strip, out_hbm, out_ref, done)


def experts_of(kernel, rows, parts, halves, hidden, *more):
    count, pieces, height, wide = parts.shape
    height_rows, width = rows.shape
    columns = 2 * hidden
    deep, tall = hidden // count, width // count // halves
    vmem, hbm = pl.BlockSpec(memory_space=pltpu.VMEM), pl.BlockSpec(memory_space=pltpu.HBM)
    return pl.pallas_call(
        kernel,
        out_shape=pltpu.HBM((height_rows, width), jnp.bfloat16),
        in_specs=[hbm, hbm] + [vmem] * len(more),
        out_specs=hbm,
        scratch_shapes=[
            pltpu.VMEM((height_rows, width), jnp.bfloat16),
            pltpu.VMEM((height_rows, width), jnp.bfloat16),
            pltpu.VMEM((count, halves, tall, columns), jnp.bfloat16),
            pltpu.VMEM((count, deep, width), jnp.bfloat16),
            pltpu.SemaphoreType.DMA((1 + pieces + width // wide,)),
            pltpu.SemaphoreType.DMA((width // columns,)),
        ],
        compiler_params=pltpu.CompilerParams(vmem_limit_bytes=32 * 1024 * 1024),
        cost_estimate=pl.CostEstimate(
            flops=6 * height_rows * width * hidden,
            bytes_accessed=count * pieces * height * wide * 2,
            transcendentals=height_rows * hidden,
        ),
    )(pltpu.with_memory_space_constraint(rows, pltpu.HBM), pltpu.with_memory_space_constraint(parts, pltpu.HBM), *more)


def shifted(array, by):
    sections = lax.axis_size(PIPE)
    return lax.ppermute(array, PIPE, [(i, (i + by) % sections) for i in range(sections)])


def picked(chosen, rows, axis):
    return lax.dot_general(
        chosen, rows, (((axis,), (0,)), ((), ())), preferred_element_type=jnp.float32
    )


def on_device(
    forward_in,
    forward_ids,
    forward_gates,
    grad_in,
    grad_ids,
    grad_gates,
    saved_input,
    saved_acts,
    norm_gain,
    weight_in,
    weight_out,
):
    grads, norm_scale = grad_in[0], norm_gain[0]
    token_count, model_width = grads.shape
    experts = lax.axis_size(("y", "zh", "c")) // 4
    capacity = token_count // experts
    hidden, columns = weight_out.shape[1], weight_in.shape[2]
    halves, places = lax.axis_size("zp"), lax.axis_size(BACK)
    rows = places * capacity

    got = exchanged(weight_pieces(weight_in[0], weight_out[0]), FAR)
    part = exchanged(got, NEAR)
    parts = lax.all_gather(part, RING, axis=0)

    grad_slot = slots(grad_ids[0], capacity)
    grad_own = grouped(grad_slot, grads)
    grad_partner = swapped_rows(grad_own)

    tokens = forward_in[0]
    fwd_slot = slots(forward_ids[0], capacity)
    fwd_own = grouped(fwd_slot, normalize(tokens, norm_scale))
    fwd_partner = swapped_rows(fwd_own)

    xs, zs, ys, far = lax.axis_size("x"), lax.axis_size("zp"), lax.axis_size("y"), lax.axis_size(FAR)
    acts = saved_acts[0, 0].reshape(ys, far, capacity, columns).transpose(1, 0, 2, 3)
    acts = exchanged(acts.reshape(far, ys * capacity, columns), FAR)
    acts = exchanged(acts, NEAR)
    acts = acts.reshape(xs, zs, ys, capacity, columns).transpose(0, 2, 1, 3, 4)

    grad_sent = for_plane(grad_own, grad_partner, experts, capacity)
    grad_rows = exchanged(grad_sent, PLANE).reshape(rows, model_width)
    fwd_sent = for_plane(fwd_own, fwd_partner, experts, capacity)
    fwd_rows = exchanged(fwd_sent, PLANE).reshape(rows, model_width)

    grad_part = experts_of(
        gradient_kernel, grad_rows, parts, halves, hidden, acts.reshape(rows, columns)
    )
    grad_back = exchanged(grad_part.reshape(places, capacity, model_width), BACK)
    fwd_part = experts_of(forward_kernel, fwd_rows, parts, halves, hidden)
    fwd_back = exchanged(fwd_part.reshape(places, capacity, model_width), BACK)

    pulled = grad_gates[0] * returned(
        grad_slot, grad_back.reshape(rows, model_width), experts, capacity
    )
    widened = saved_input[0].astype(jnp.float32)
    inverse_rms = lax.rsqrt(jnp.mean(widened * widened, axis=-1, keepdims=True) + epsilon)
    unit_rows = widened * inverse_rms
    weighted = pulled * norm_scale
    through = grads.astype(jnp.float32) + inverse_rms * (
        weighted - unit_rows * jnp.mean(weighted * unit_rows, axis=-1, keepdims=True)
    )
    grad_out = shifted(through.astype(jnp.bfloat16)[None], -1)
    combined = forward_gates[0] * returned(
        fwd_slot, fwd_back.reshape(rows, model_width), experts, capacity
    )
    moved = (tokens.astype(jnp.float32) + combined).astype(jnp.bfloat16)
    forward_out = shifted(moved[None], 1)
    return (forward_out, grad_out)


def solution(mesh):
    fine = Mesh(mesh.devices.reshape(4, 4, 2, 4, 4, 2), ("x", "zj", "zp", "y", "zh", "c"))
    expert = ("y", "zh", "c")
    rows = P(PIPE, expert, None)
    placed = (rows,) * 7 + (
        P(PIPE, expert, None, None),
        P(PIPE, None),
        P(expert, None, None),
        P(expert, None, None),
    )
    return jax.shard_map(
        on_device, mesh=fine, in_specs=placed, out_specs=(rows, rows), check_vma=False
    )
```

```python
import jax
import jax.numpy as jnp
import numpy as np
from jax import lax
from jax.experimental import pallas as pl
from jax.experimental.pallas import tpu as pltpu
from jax.sharding import Mesh, PartitionSpec as P

epsilon = 1e-06
PIPE = ("x", "zj", "zp")
FAR = ("zh", "c")
NEAR = ("x", "zp")
PLANE = ("x", "y")
BACK = ("x", "y", "zp")
RING = ("zh", "zj", "c")


def normalize(tokens, norm_scale):
    widened = tokens.astype(jnp.float32)
    inverse_rms = lax.rsqrt(jnp.mean(widened * widened, axis=-1, keepdims=True) + epsilon)
    return (widened * inverse_rms * norm_scale).astype(jnp.bfloat16)


def slots(route_ids, capacity):
    ids = route_ids[:, 0]
    tokens = ids.shape[0]
    row = lax.broadcasted_iota(jnp.int32, (tokens, tokens), 0)
    column = lax.broadcasted_iota(jnp.int32, (tokens, tokens), 1)
    earlier = (ids[:, None] == ids[None, :]) & (column < row)
    return ids * capacity + jnp.sum(earlier.astype(jnp.int32), axis=1)


def grouped(slot, rows):
    chosen = slot[:, None] == lax.broadcasted_iota(jnp.int32, (rows.shape[0],) * 2, 1)
    return picked(chosen.astype(jnp.bfloat16), rows, 0).astype(jnp.bfloat16)


def returned(slot, rows, experts, capacity):
    xs, ys, zs = lax.axis_size("x"), lax.axis_size("y"), lax.axis_size("zp")
    pairs = experts // ys
    x, y, _, rank = np.indices((xs, ys, zs, capacity))
    place = ((y * pairs + x // (xs // pairs)) * capacity + rank).reshape(1, -1)
    chosen = slot[:, None] == jnp.asarray(place, jnp.int32)
    return picked(chosen.astype(jnp.bfloat16), rows, 1)


def swapped_rows(rows):
    zs = lax.axis_size("zp")
    return lax.ppermute(rows, "zp", [(i, zs - 1 - i) for i in range(zs)])


def for_plane(own, partner, experts, capacity):
    xs, ys, zs = lax.axis_size("x"), lax.axis_size("y"), lax.axis_size("zp")
    pairs = experts // ys
    width = own.shape[1]
    even = lax.axis_index("zp") == 0
    both = jnp.stack([jnp.where(even, own, partner), jnp.where(even, partner, own)])
    both = both.reshape(zs, ys, pairs, capacity, width).transpose(2, 1, 0, 3, 4)
    both = jnp.broadcast_to(both[:, None], (pairs, xs // pairs, ys, zs, capacity, width))
    return both.reshape(xs * ys, zs * capacity, width)


def exchanged(rows, axes):
    return lax.all_to_all(rows, axes, split_axis=0, concat_axis=0, tiled=True)


def weight_pieces(weight_in, weight_out):
    width, columns = weight_in.shape
    hidden = weight_out.shape[0]
    far, run, parts = lax.axis_size(FAR), lax.axis_size("zj"), lax.axis_size(RING)
    zh, cs = lax.axis_size("zh"), lax.axis_size("c")
    strips, halves = lax.axis_size("x"), lax.axis_size("zp")
    tall, wide = width // parts // halves, columns // strips
    deep = hidden // parts
    pieces = width // columns
    j, x, half = lax.axis_index("zj"), lax.axis_index("x"), lax.axis_index("zp")
    first = lax.dynamic_slice(
        weight_in.reshape(zh, run, cs, halves, tall, columns),
        (0, j, 0, half, 0, x * wide),
        (zh, 1, cs, 1, tall, wide),
    ).reshape(far, tall, wide)
    piece = jnp.minimum(x * halves + half, pieces - 1)
    second = lax.dynamic_slice(
        weight_out.reshape(zh, run, cs, deep, width),
        (0, j, 0, 0, piece * columns),
        (zh, 1, cs, deep, columns),
    )
    second = second.reshape(far, deep, strips, wide).transpose(0, 2, 1, 3)
    return jnp.concatenate([first, second.reshape(far, strips * deep, wide)], axis=1)


def weight_copies(parts_ref, first_ref, second_ref, sems):
    _, halves, tall, columns = first_ref.shape
    _, deep, width = second_ref.shape
    wide = parts_ref.shape[3]
    strips = columns // wide
    first_copies = [
        pltpu.make_async_copy(
            parts_ref.at[:, s * halves + h, pl.ds(0, tall), :],
            first_ref.at[:, h, :, pl.ds(s * wide, wide)],
            sems.at[1 + s * halves + h],
        )
        for s in range(strips)
        for h in range(halves)
    ]
    second_copies = [
        pltpu.make_async_copy(
            parts_ref.at[:, q // strips, pl.ds(tall + q % strips * deep, deep), :],
            second_ref.at[:, :, pl.ds(q * wide, wide)],
            sems.at[1 + strips * halves + q],
        )
        for q in range(width // wide)
    ]
    return first_copies, second_copies


def written(strip, out_hbm, out_ref, done):
    width = out_ref.shape[1] // done.shape[0]
    copies = []
    for q in range(done.shape[0]):
        part = slice(q * width, (q + 1) * width)
        out_ref[:, part] = strip(part).astype(jnp.bfloat16)
        columns_of = pl.ds(q * width, width)
        copies.append(
            pltpu.make_async_copy(out_ref.at[:, columns_of], out_hbm.at[:, columns_of], done.at[q])
        )
        copies[-1].start()
    for copy in copies:
        copy.wait()


def forward_kernel(rows_hbm, parts_ref, out_hbm, rows_ref, out_ref, first_ref, second_ref, sems, done):
    parts, halves, tall, columns = first_ref.shape
    _, deep, _ = second_ref.shape
    hidden = parts * deep
    first_copies, second_copies = weight_copies(parts_ref, first_ref, second_ref, sems)
    rows_copy = pltpu.make_async_copy(rows_hbm, rows_ref, sems.at[0])
    for copy in [rows_copy] + first_copies + second_copies:
        copy.start()
    for copy in [rows_copy] + first_copies:
        copy.wait()
    first = first_ref[...].reshape(parts * halves * tall, columns)
    projected = jnp.dot(rows_ref[...], first, preferred_element_type=jnp.float32)
    gate, up = projected[:, :hidden], projected[:, hidden:]
    mixed = (gate / (1.0 + jnp.exp(-gate)) * up).astype(jnp.bfloat16)
    for copy in second_copies:
        copy.wait()

    def strip(columns_of):
        second = second_ref[:, :, columns_of].reshape(hidden, -1)
        return jnp.dot(mixed, second, preferred_element_type=jnp.float32)

    written(strip, out_hbm, out_ref, done)


def gradient_kernel(
    rows_hbm, parts_ref, acts_ref, out_hbm, rows_ref, out_ref, first_ref, second_ref, sems, done
):
    parts, _, _, columns = first_ref.shape
    _, deep, width = second_ref.shape
    hidden = parts * deep
    first_copies, second_copies = weight_copies(parts_ref, first_ref, second_ref, sems)
    rows_copy = pltpu.make_async_copy(rows_hbm, rows_ref, sems.at[0])
    for copy in [rows_copy] + second_copies + first_copies:
        copy.start()
    for copy in [rows_copy] + second_copies:
        copy.wait()
    turned = (((1,), (1,)), ((), ()))
    second = second_ref[...].reshape(hidden, width)
    hidden_grad = lax.dot_general(rows_ref[...], second, turned, preferred_element_type=jnp.float32)
    gate_act = acts_ref[:, :hidden].astype(jnp.float32)
    up_act = acts_ref[:, hidden:].astype(jnp.float32)
    squashed = 1.0 / (1.0 + jnp.exp(-gate_act))
    gate_grad = hidden_grad * up_act * squashed * (1.0 + gate_act * (1.0 - squashed))
    up_grad = hidden_grad * gate_act * squashed
    joined = jnp.concatenate([gate_grad.astype(jnp.bfloat16), up_grad.astype(jnp.bfloat16)], axis=1)
    for copy in first_copies:
        copy.wait()

    first = first_ref[...].reshape(width, columns)

    def strip(columns_of):
        return lax.dot_general(
            joined, first[columns_of, :], turned, preferred_element_type=jnp.float32
        )

    written(strip, out_hbm, out_ref, done)


def experts_of(kernel, rows, parts, halves, hidden, *more):
    count, pieces, height, wide = parts.shape
    height_rows, width = rows.shape
    columns = 2 * hidden
    deep, tall = hidden // count, width // count // halves
    vmem, hbm = pl.BlockSpec(memory_space=pltpu.VMEM), pl.BlockSpec(memory_space=pltpu.HBM)
    return pl.pallas_call(
        kernel,
        out_shape=pltpu.HBM((height_rows, width), jnp.bfloat16),
        in_specs=[hbm, hbm] + [vmem] * len(more),
        out_specs=hbm,
        scratch_shapes=[
            pltpu.VMEM((height_rows, width), jnp.bfloat16),
            pltpu.VMEM((height_rows, width), jnp.bfloat16),
            pltpu.VMEM((count, halves, tall, columns), jnp.bfloat16),
            pltpu.VMEM((count, deep, width), jnp.bfloat16),
            pltpu.SemaphoreType.DMA((1 + pieces + width // wide,)),
            pltpu.SemaphoreType.DMA((width // columns,)),
        ],
        compiler_params=pltpu.CompilerParams(vmem_limit_bytes=32 * 1024 * 1024),
        cost_estimate=pl.CostEstimate(
            flops=6 * height_rows * width * hidden,
            bytes_accessed=count * pieces * height * wide * 2,
            transcendentals=height_rows * hidden,
        ),
    )(pltpu.with_memory_space_constraint(rows, pltpu.HBM), pltpu.with_memory_space_constraint(parts, pltpu.HBM), *more)


def moved_acts(acts):
    axes = ("x", "zp", "zh", "c")
    xs, zs, blocks, cs = (lax.axis_size(axis) for axis in axes)
    x, zp, zh, c = (lax.axis_index(axis) for axis in axes)

    def flat(a, b, k, m):
        return ((a * zs + b) * blocks + k) * cs + m

    got = []
    for dk in range(blocks):
        for dm in range(cs):
            pairs = [
                (flat(i, j, k, m), flat(k, m, (i + dk) % blocks, (j + dm) % cs))
                for i, j, k, m in np.ndindex(xs, zs, blocks, cs)
            ]
            piece = lax.dynamic_index_in_dim(
                acts, (x + dk) % blocks * cs + (zp + dm) % cs, 0, keepdims=False
            )
            got.append(lax.ppermute(piece, axes, pairs))
    got = jnp.stack(got)
    return jnp.stack(
        [
            lax.dynamic_index_in_dim(
                got, (zh - i) % blocks * cs + (c - j) % cs, 0, keepdims=False
            )
            for i in range(xs)
            for j in range(zs)
        ]
    )


def shifted(array, by):
    sections = lax.axis_size(PIPE)
    return lax.ppermute(array, PIPE, [(i, (i + by) % sections) for i in range(sections)])


def picked(chosen, rows, axis):
    return lax.dot_general(
        chosen, rows, (((axis,), (0,)), ((), ())), preferred_element_type=jnp.float32
    )


def on_device(
    forward_in,
    forward_ids,
    forward_gates,
    grad_in,
    grad_ids,
    grad_gates,
    saved_input,
    saved_acts,
    norm_gain,
    weight_in,
    weight_out,
):
    grads, norm_scale = grad_in[0], norm_gain[0]
    token_count, model_width = grads.shape
    experts = lax.axis_size(("y", "zh", "c")) // 4
    capacity = token_count // experts
    hidden, columns = weight_out.shape[1], weight_in.shape[2]
    halves, places = lax.axis_size("zp"), lax.axis_size(BACK)
    rows = places * capacity

    got = exchanged(weight_pieces(weight_in[0], weight_out[0]), FAR)
    part = exchanged(got, NEAR)
    parts = lax.all_gather(part, RING, axis=0)

    grad_slot = slots(grad_ids[0], capacity)
    grad_own = grouped(grad_slot, grads)
    grad_partner = swapped_rows(grad_own)

    tokens = forward_in[0]
    fwd_slot = slots(forward_ids[0], capacity)
    fwd_own = grouped(fwd_slot, normalize(tokens, norm_scale))
    fwd_partner = swapped_rows(fwd_own)

    xs, zs, ys, far = lax.axis_size("x"), lax.axis_size("zp"), lax.axis_size("y"), lax.axis_size(FAR)
    acts = saved_acts[0, 0].reshape(ys, far, capacity, columns).transpose(1, 0, 2, 3)
    acts = moved_acts(acts.reshape(far, ys * capacity, columns))
    acts = acts.reshape(xs, zs, ys, capacity, columns).transpose(0, 2, 1, 3, 4)

    grad_sent = for_plane(grad_own, grad_partner, experts, capacity)
    grad_rows = exchanged(grad_sent, PLANE).reshape(rows, model_width)
    fwd_sent = for_plane(fwd_own, fwd_partner, experts, capacity)
    fwd_rows = exchanged(fwd_sent, PLANE).reshape(rows, model_width)

    grad_part = experts_of(
        gradient_kernel, grad_rows, parts, halves, hidden, acts.reshape(rows, columns)
    )
    grad_back = exchanged(grad_part.reshape(places, capacity, model_width), BACK)
    fwd_part = experts_of(forward_kernel, fwd_rows, parts, halves, hidden)
    fwd_back = exchanged(fwd_part.reshape(places, capacity, model_width), BACK)

    pulled = grad_gates[0] * returned(
        grad_slot, grad_back.reshape(rows, model_width), experts, capacity
    )
    widened = saved_input[0].astype(jnp.float32)
    inverse_rms = lax.rsqrt(jnp.mean(widened * widened, axis=-1, keepdims=True) + epsilon)
    unit_rows = widened * inverse_rms
    weighted = pulled * norm_scale
    through = grads.astype(jnp.float32) + inverse_rms * (
        weighted - unit_rows * jnp.mean(weighted * unit_rows, axis=-1, keepdims=True)
    )
    grad_out = shifted(through.astype(jnp.bfloat16)[None], -1)
    combined = forward_gates[0] * returned(
        fwd_slot, fwd_back.reshape(rows, model_width), experts, capacity
    )
    moved = (tokens.astype(jnp.float32) + combined).astype(jnp.bfloat16)
    forward_out = shifted(moved[None], 1)
    return (forward_out, grad_out)


def solution(mesh):
    fine = Mesh(mesh.devices.reshape(4, 4, 2, 4, 4, 2), ("x", "zj", "zp", "y", "zh", "c"))
    expert = ("y", "zh", "c")
    rows = P(PIPE, expert, None)
    placed = (rows,) * 7 + (
        P(PIPE, expert, None, None),
        P(PIPE, None),
        P(expert, None, None),
        P(expert, None, None),
    )
    return jax.shard_map(
        on_device, mesh=fine, in_specs=placed, out_specs=(rows, rows), check_vma=False
    )
```
